32 devices in a mesh: chip: 2 (over y), board: 4 (over z), cuts: 4 (over x, core).
Axes of the slice: x: 2, y: 2, z: 4, core: 2. Of those that a mesh axis runs over, the one named last changes fastest.
Arguments:
- features: bfloat16 [32, 2048, 1024], P(('chip', 'board', 'cuts')), may hold values from -6 to 6
- targets: bfloat16 [32, 2048, 256], P(('chip', 'board', 'cuts')), may hold values from -24 to 24
- lower_weight: bfloat16 [32, 1024, 512], P(('chip', 'board', 'cuts')), may hold values from -0.1875 to 0.1875
- head_weight: float32 [32, 512, 256], P(('chip', 'board', 'cuts')), may hold values from -0.25 to 0.25
- batch_rows: int32 [32, 2, 1024], P(('chip', 'board', 'cuts')), may hold values from 0 to 2047
- sample_counts: int32 [32], P(('chip', 'board', 'cuts')), may hold values from 1 to 1000
- cluster_ids: int32 [32], P(('chip', 'board', 'cuts')), may hold values from 0 to 7, as said below
Outputs:
- cluster_step: float32 [32, 512, 256], P(('chip', 'board', 'cuts'))
The draws below stay inside these ranges and needn't reach their ends.
Inputs may be any that keep to these rules, and one draw needn't show every extreme that they name: `cluster_ids`: every one of the 8 clusters has at least one client.
All inputs are finite; a program needn't handle non-finite values.
Results may differ from the reference program's by a relative error of at most 0.0003.
Values sent between devices are 32-bit elements; how exact they have to be, the bound alone decides.
No kernel may reach another device: no remote copies, remote signals or barrier semaphores. Data moves between devices by JAX's collectives and lax.ppermute only.
A program may use at most 64 MiB of HBM per device.

```python
import jax
import jax.numpy as jnp
from jax import lax

IN = 1024
HID = 512
OUT = 256
CLUSTERS = 8
STEPS = 2
POOL = 2048
ROWS = 1024
CLIENTS = 32


def draw_cluster_ids(key, part):
    first = jax.random.fold_in(key, 11)
    second = jax.random.fold_in(key, 23)
    drawn = jax.random.randint(first, (CLIENTS,), 0, CLUSTERS, dtype=jnp.int32)
    order = jax.random.permutation(second, CLIENTS)
    return drawn.at[order[:CLUSTERS]].set(jnp.arange(CLUSTERS, dtype=jnp.int32))


def with_ends(values, rng, smallest, largest):
    index_at = [jax.random.randint(jax.random.fold_in(rng, axis), (), 0, length) for axis, length in enumerate(values.shape)]
    widest = values.shape.index(max(values.shape))
    neighbour = index_at[:widest] + [(index_at[widest] + 1) % values.shape[widest]] + index_at[widest + 1:]
    return values.at[tuple(index_at)].set(smallest).at[tuple(neighbour)].set(largest)


def level_of(key, shape, cuts, low, largest):
    def one(dim, parts):
        draws = jax.random.uniform(jax.random.fold_in(jax.random.fold_in(key, 6), dim), (parts,), jnp.float32, low / len(cuts), largest / len(cuts))
        return jnp.repeat(jnp.exp(draws), shape[dim] // parts).reshape((-1,) + (1,) * (len(shape) - dim - 1))

    gain = one(*cuts[0])
    for cut in cuts[1:]:
        gain = gain * one(*cut)
    return gain


def centred(key, shape, width, limit, cuts=(), kind=jnp.bfloat16):
    result = jax.random.normal(key, shape, jnp.float32) * width
    if len(cuts) > 0:
        result = level_of(key, shape, cuts, -0.22, 0.18) * result
    return jnp.clip(result, min=-limit, max=limit).astype(kind)


def setup_inputs(seed: int = 0) -> dict:
    arg_keys = jax.random.split(jax.random.key(seed), 8)
    return {
        "features": centred(arg_keys[0], (CLIENTS, POOL, IN), 1.0, 6.0, ((0, 32),)),
        "targets": centred(arg_keys[1], (CLIENTS, POOL, OUT), 4.0, 24.0, ((0, 32),)),
        "lower_weight": centred(arg_keys[2], (CLIENTS, IN, HID), IN ** -0.5, 0.1875, ((0, 32),)),
        "head_weight": centred(arg_keys[3], (CLIENTS, HID, OUT), HID ** -0.5, 0.25, ((0, 32),), jnp.float32),
        "batch_rows": with_ends(jax.random.randint(arg_keys[4], (CLIENTS, STEPS, ROWS), 0, POOL), jax.random.fold_in(arg_keys[4], 1), 0, POOL - 1).astype(jnp.int32),
        "sample_counts": with_ends(jax.random.randint(arg_keys[5], (CLIENTS,), 1, 1001), jax.random.fold_in(arg_keys[5], 1), 1, 1000).astype(jnp.int32),
        "cluster_ids": draw_cluster_ids(jax.random.fold_in(arg_keys[7], 71), 0),
    }


LR = 0.5


def one_client(args):
    feats, targs, lower, head, rows = args
    hidden = jnp.tanh(jnp.dot(feats, lower, preferred_element_type=jnp.float32))
    weight = head
    for step in range(STEPS):
        picked = jnp.take(hidden, rows[step], axis=0)
        wanted = jnp.take(targs, rows[step], axis=0).astype(jnp.float32)
        err = jnp.dot(picked, weight, precision=lax.Precision.HIGHEST) - wanted
        grad = jnp.dot(picked.T, err, precision=lax.Precision.HIGHEST) / ROWS
        weight = weight - LR * grad
    return weight - head


def reference(features, targets, lower_weight, head_weight, batch_rows, sample_counts, cluster_ids):
    deltas = lax.map(one_client, (features, targets, lower_weight, head_weight, batch_rows))
    onehot = (cluster_ids[:, None] == jnp.arange(CLUSTERS, dtype=jnp.int32)[None, :]).astype(jnp.float32)
    weighted = onehot * sample_counts.astype(jnp.float32)[:, None]
    flat = deltas.reshape(CLIENTS, HID * OUT)
    sums = jnp.dot(weighted.T, flat, precision=lax.Precision.HIGHEST)
    counts = jnp.sum(weighted, axis=0)
    mine = jnp.take(sums, cluster_ids, axis=0).reshape(CLIENTS, HID, OUT)
    denom = jnp.take(counts, cluster_ids, axis=0)
    return mine / (LR * denom)[:, None, None]
```

```python
import functools

import jax
import jax.numpy as jnp
from jax import lax
from jax.experimental import pallas as pl
from jax.experimental.pallas import tpu as pltpu
from jax.sharding import PartitionSpec as P

LR = 0.5
CLUSTERS = 8
LANES = 128
SUB = 8
AXES = ("chip", "board", "cuts")
F32 = jnp.float32
BF16 = jnp.bfloat16


def halves(value):
    high = value.astype(BF16)
    return high, (value - high.astype(F32)).astype(BF16)


def product(a, b, contract):
    dims = (contract, ((), ()))
    dot = functools.partial(lax.dot_general, dimension_numbers=dims, preferred_element_type=F32)
    return dot(a[0], b[0]) + (dot(a[0], b[1]) + dot(a[1], b[0]))


def client_kernel(
    rows_ref, count_ref, cluster_ref, features_ref, lower_ref, targets_ref, head_ref, out_ref,
    feat, low, targ, start, pool, picked, grad, weight, arrived, *, shares, chunk,
):
    pool_rows, hidden = feat.shape[0], low.shape[1]
    steps, count_rows = rows_ref.shape
    outs = targ.shape[1]
    blocks, tblocks = hidden // LANES, outs // LANES

    def part(i):
        at = pl.ds(i * chunk, chunk)
        return pltpu.make_async_copy(features_ref.at[0, at], feat.at[at], arrived.at[i])

    chunks = pool_rows // chunk
    whole = [
        pltpu.make_async_copy(lower_ref.at[0], low, arrived.at[chunks]),
        pltpu.make_async_copy(targets_ref.at[0], targ, arrived.at[chunks + 1]),
        pltpu.make_async_copy(head_ref.at[0], start, arrived.at[chunks + 2]),
    ]
    whole[0].start()
    for i in range(chunks):
        part(i).start()
    whole[1].start()
    whole[2].start()
    whole[0].wait()
    whole[1].wait()

    @pl.loop(0, chunks)
    def _(i):
        part(i).wait()
        at = pl.ds(pl.multiple_of(i * chunk, chunk), chunk)
        h = jnp.tanh(jnp.dot(feat[at, :], low[...], preferred_element_type=F32))
        t = targ[at, :].astype(F32)
        for k in range(blocks):
            pool[pl.ds(i * chunk * SUB + k, chunk, stride=SUB), :] = h[:, k * LANES:(k + 1) * LANES]
        for k in range(tblocks):
            pool[pl.ds(i * chunk * SUB + blocks + k, chunk, stride=SUB), :] = t[:, k * LANES:(k + 1) * LANES]

    whole[2].wait()
    total = steps * (count_rows // chunk)

    def gather(slot, i):
        step, at = i // (count_rows // chunk), (i % (count_rows // chunk)) * chunk
        for r in range(chunk):
            row = rows_ref[step, at + r]
            picked[slot, r * SUB:(r + 1) * SUB, :] = pool[pl.ds(pl.multiple_of(row * SUB, SUB), SUB), :]

    def one(slot):
        view = picked.at[slot]
        h = halves(jnp.concatenate([view[pl.ds(k, chunk, stride=SUB), :] for k in range(blocks)], axis=1))
        t = jnp.concatenate([view[pl.ds(blocks + k, chunk, stride=SUB), :] for k in range(tblocks)], axis=1)
        err = product(h, (weight[0], weight[1]), ((1,), (0,))) - t
        grad[...] += product(h, halves(err), ((0,), (0,)))

    def load_weight(value):
        high, rest = halves(value)
        weight[0], weight[1] = high, rest

    load_weight(start[...])
    grad[...] = jnp.zeros_like(grad)
    gather(0, 0)
    per_step = count_rows // chunk
    for step in range(steps):
        @pl.loop(0, per_step // 2)
        def _(j):
            i = step * per_step + 2 * j
            gather(1, i + 1)
            one(0)
            gather(0, jnp.minimum(i + 2, total - 1))
            one(1)
        if step + 1 < steps:
            load_weight(start[...] - (LR / count_rows) * grad[...])

    each = hidden // shares
    width = tblocks * each + 1
    count = count_ref[0].astype(F32)
    scale = -(LR / count_rows)
    lane = lax.broadcasted_iota(jnp.int32, (1, LANES), 1)
    note = jnp.where(lane < LANES // 2, cluster_ref[0].astype(F32), count)
    for s in range(shares):
        for k in range(tblocks):
            out_ref[s * width + k * each:s * width + (k + 1) * each, :] = (
                grad[s * each:(s + 1) * each, k * LANES:(k + 1) * LANES] * scale
            )
        out_ref[(s + 1) * width - 1:(s + 1) * width, :] = note


def cluster_kernel(in_ref, out_ref, *, shares):
    each, outs = out_ref.shape[1], out_ref.shape[2]
    tblocks = outs // LANES
    data = tblocks * each
    width = data + 1
    full = (data, LANES)
    sums = [jnp.zeros(full, F32)] * CLUSTERS
    counts = [jnp.zeros((1, LANES), F32)] * CLUSTERS
    ids = []
    for j in range(shares):
        note = in_ref[(j + 1) * width - 1:(j + 1) * width, :]
        ident = jnp.broadcast_to(note[:, 0:1], (1, LANES))
        count = jnp.broadcast_to(note[:, LANES - 1:LANES], (1, LANES))
        ids.append(ident)
        delta = in_ref[j * width:j * width + data, :]
        for c in range(CLUSTERS):
            weight = jnp.where(ident == c, count, 0.0)
            counts[c] = counts[c] + weight
            sums[c] = sums[c] + weight * delta
    sums = [total / (LR * count) for total, count in zip(sums, counts)]
    for j in range(shares):
        mine = sums[0]
        for c in range(1, CLUSTERS):
            mine = jnp.where(ids[j] == c, sums[c], mine)
        for k in range(tblocks):
            out_ref[j, :, k * LANES:(k + 1) * LANES] = mine[k * each:(k + 1) * each]


def on_device(features, targets, lower_weight, head_weight, batch_rows, sample_counts, cluster_ids):
    shares = lax.axis_size(AXES)
    pool_rows, inputs = features.shape[1:]
    hidden, outs = head_weight.shape[1:]
    chunk = 256
    each = hidden // shares
    tblocks = outs // LANES
    width = tblocks * each + 1
    smem = pl.BlockSpec(memory_space=pltpu.SMEM)
    hbm = pl.BlockSpec(memory_space=pltpu.HBM)
    vmem = pl.BlockSpec(memory_space=pltpu.VMEM)
    outgoing = pl.pallas_call(
        functools.partial(client_kernel, shares=shares, chunk=chunk),
        out_shape=jax.ShapeDtypeStruct((shares * width, LANES), F32),
        in_specs=[smem, smem, smem, hbm, hbm, hbm, hbm],
        out_specs=vmem,
        scratch_shapes=[
            pltpu.VMEM((pool_rows, inputs), BF16),
            pltpu.VMEM((inputs, hidden), BF16),
            pltpu.VMEM((pool_rows, outs), BF16),
            pltpu.VMEM((hidden, outs), F32),
            pltpu.VMEM((pool_rows * SUB, LANES), F32),
            pltpu.VMEM((2, chunk * SUB, LANES), F32),
            pltpu.VMEM((hidden, outs), F32),
            pltpu.VMEM((2, hidden, outs), BF16),
            pltpu.SemaphoreType.DMA((pool_rows // chunk + 3,)),
        ],
        compiler_params=pltpu.CompilerParams(vmem_limit_bytes=40 << 20),
        name="client",
    )(batch_rows[0], sample_counts, cluster_ids, features, lower_weight, targets, head_weight)
    arrived = lax.all_to_all(outgoing.reshape(shares * width, 1, LANES), AXES, split_axis=0, concat_axis=0, tiled=True)
    back = pl.pallas_call(
        functools.partial(cluster_kernel, shares=shares),
        out_shape=jax.ShapeDtypeStruct((shares, each, outs), F32),
        in_specs=[vmem],
        out_specs=vmem,
        name="cluster",
    )(arrived.reshape(shares * width, LANES))
    mine = lax.all_to_all(back, AXES, split_axis=0, concat_axis=0, tiled=True)
    return mine.reshape(head_weight.shape)


def solution(mesh):
    whole = P(AXES, None, None)
    return jax.shard_map(
        on_device,
        mesh=mesh,
        in_specs=(whole, whole, whole, whole, whole, P(AXES), P(AXES)),
        out_specs=whole,
        check_vma=False,
    )
```

```python
import functools

import jax
import jax.numpy as jnp
from jax import lax
from jax.experimental import pallas as pl
from jax.experimental.pallas import tpu as pltpu
from jax.sharding import PartitionSpec as P

LR = 0.5
CLUSTERS = 8
LANES = 128
SUB = 8
PITCH = 9
VMEM_LIMIT = 65_500_000
AXES = ("chip", "board", "cuts")
F32 = jnp.float32
BF16 = jnp.bfloat16


def halves(value):
    high = value.astype(BF16)
    return high, (value - high.astype(F32)).astype(BF16)


def client_kernel(
    rows_hbm, count_ref, cluster_ref, features_ref, lower_ref, targets_ref, head_ref, out_ref,
    rows_ref, feat, low, targ, start, pool, picked_a, picked_b,
    first, total, begin, weight, arrived, *, shares, chunk,
):
    pool_rows, hidden = feat.shape[0], low.shape[1]
    steps, count_rows = rows_hbm.shape[1:]
    outs = targ.shape[1]
    blocks, tblocks = hidden // LANES, outs // LANES
    chunks = pool_rows // chunk
    scale = -(LR / count_rows)

    def part(i):
        at = pl.ds(i * chunk, chunk)
        return pltpu.make_async_copy(features_ref.at[0, at], feat.at[at], arrived.at[i])

    def whole(source, target, i):
        return pltpu.make_async_copy(source, target, arrived.at[chunks + i])

    low_copy = whole(lower_ref.at[0], low, 0)
    targ_copy = whole(targets_ref.at[0], targ, 1)
    late = [
        whole(head_ref.at[0], start, 2),
        *[whole(rows_hbm.at[0, s], rows_ref.at[pl.ds(s * count_rows, count_rows)], 3 + s) for s in range(steps)],
    ]
    ahead = 2
    low_copy.start()
    for i in range(ahead):
        part(i).start()
    low_copy.wait()
    for i in range(ahead, 2 * ahead):
        part(i).start()

    def sample(i, with_targets):
        part(i).wait()
        at = pl.ds(pl.multiple_of(i * chunk, chunk), chunk)
        h = jnp.tanh(jnp.dot(feat[at, :], low[...], preferred_element_type=F32))
        for k in range(blocks):
            pool[pl.ds(i * chunk * PITCH + k, chunk, stride=PITCH), :] = h[:, k * LANES:(k + 1) * LANES]
        for j in range(2 if with_targets else 0):
            c = 2 * i - chunks + j
            t = targ[pl.ds(pl.multiple_of(c * chunk, chunk), chunk), :].astype(F32)
            for k in range(tblocks):
                pool[pl.ds(c * chunk * PITCH + blocks + k, chunk, stride=PITCH), :] = t[:, k * LANES:(k + 1) * LANES]

    @pl.loop(0, chunks // 2)
    def _(i):
        part(i + 2 * ahead).start()

        @pl.when(i == 1)
        def _():
            targ_copy.start()
            for copy in late:
                copy.start()

        sample(i, False)

    targ_copy.wait()

    @pl.loop(chunks // 2, chunks)
    def _(i):
        @pl.when(i + 2 * ahead < chunks)
        def _():
            part(i + 2 * ahead).start()

        sample(i, True)

    for copy in late:
        copy.wait()

    per_step = count_rows // chunk

    def pick(i, into):
        for r in range(chunk):
            row = rows_ref[i * chunk + r]
            into[r * PITCH:r * PITCH + SUB, :] = pool[pl.ds(row * PITCH, SUB), :]

    def picks(source):
        h = jnp.concatenate([source[pl.ds(k, chunk, stride=PITCH), :] for k in range(blocks)], axis=1)
        t = jnp.concatenate([source[pl.ds(blocks + k, chunk, stride=PITCH), :] for k in range(tblocks)], axis=1)
        return (*halves(h), t.astype(BF16))

    def load_weight(value):
        w_high, w_rest = halves(value)
        weight[:, :hidden] = w_high
        weight[:, hidden:2 * hidden] = w_rest
        weight[:, 2 * hidden:3 * hidden] = w_high

    def errors(h, rest, t):
        e = lax.dot_general(
            weight[...], jnp.concatenate([h, h, rest, t], axis=1), (((1,), (1,)), ((), ())), preferred_element_type=F32
        )
        return halves(e)

    start_t = start[...].T
    begin[...] = start_t
    load_weight(start_t)
    row_at = lax.broadcasted_iota(jnp.int32, (outs, outs), 0)
    lane_at = lax.broadcasted_iota(jnp.int32, (outs, outs), 1)
    weight[:, 3 * hidden:] = jnp.where(row_at == lane_at, -1.0, 0.0).astype(BF16)
    total[...] = jnp.zeros_like(total)
    pick(0, picked_a)
    last = steps * per_step - 1

    for step in range(steps):
        @pl.loop(0, per_step // 2)
        def _(j):
            i = step * per_step + 2 * j
            pick(i + 1, picked_b)
            h_a, rest_a, t_a = picks(picked_a)
            e_a, d_a = errors(h_a, rest_a, t_a)
            h_b, rest_b, t_b = picks(picked_b)
            e_b, d_b = errors(h_b, rest_b, t_b)
            total[...] += jnp.dot(
                jnp.concatenate([e_a, d_a, e_a, e_b, d_b, e_b], axis=1),
                jnp.concatenate([h_a, h_a, rest_a, h_b, h_b, rest_b], axis=0),
                preferred_element_type=F32,
            )
            pick(jnp.minimum(i + 2, last), picked_a)

        if step + 1 < steps:
            load_weight(begin[...] + scale * total[...])
    first[...] = total[...].T

    each = hidden // shares
    width = tblocks * each + 1
    lane = lax.broadcasted_iota(jnp.int32, (1, LANES), 1)
    note = jnp.where(lane < LANES // 2, cluster_ref[0], count_ref[0]).astype(F32)
    for s in range(shares):
        for k in range(tblocks):
            out_ref[s * width + k * each:s * width + (k + 1) * each, :] = (
                first[s * each:(s + 1) * each, k * LANES:(k + 1) * LANES] * scale
            )
        out_ref[(s + 1) * width - 1:(s + 1) * width, :] = note


def cluster_kernel(in_ref, out_ref, *, shares):
    each, outs = out_ref.shape[1], out_ref.shape[2]
    tblocks = outs // LANES
    data = tblocks * each
    width = data + 1
    full = (data, LANES)
    sums = [jnp.zeros(full, F32)] * CLUSTERS
    counts = [jnp.zeros((1, LANES), F32)] * CLUSTERS
    ids = []
    for j in range(shares):
        note = in_ref[(j + 1) * width - 1:(j + 1) * width, :]
        ident = jnp.broadcast_to(note[:, 0:1], (1, LANES))
        count = jnp.broadcast_to(note[:, LANES - 1:LANES], (1, LANES))
        ids.append(ident)
        delta = in_ref[j * width:j * width + data, :]
        for c in range(CLUSTERS):
            weight = jnp.where(ident == c, count, 0.0)
            counts[c] = counts[c] + weight
            sums[c] = sums[c] + weight * delta
    sums = [total / (LR * count) for total, count in zip(sums, counts)]
    for j in range(shares):
        mine = sums[0]
        for c in range(1, CLUSTERS):
            mine = jnp.where(ids[j] == c, sums[c], mine)
        for k in range(tblocks):
            out_ref[j, :, k * LANES:(k + 1) * LANES] = mine[k * each:(k + 1) * each]


def on_device(features, targets, lower_weight, head_weight, batch_rows, sample_counts, cluster_ids):
    shares = lax.axis_size(AXES)
    pool_rows, inputs = features.shape[1:]
    hidden, outs = head_weight.shape[1:]
    chunk = 256
    each = hidden // shares
    tblocks = outs // LANES
    width = tblocks * each + 1
    smem = pl.BlockSpec(memory_space=pltpu.SMEM)
    hbm = pl.BlockSpec(memory_space=pltpu.HBM)
    vmem = pl.BlockSpec(memory_space=pltpu.VMEM)
    steps, count_rows = batch_rows.shape[1:]
    outgoing = pl.pallas_call(
        functools.partial(client_kernel, shares=shares, chunk=chunk),
        out_shape=jax.ShapeDtypeStruct((shares * width, LANES), F32),
        in_specs=[hbm, smem, smem, hbm, hbm, hbm, hbm],
        out_specs=vmem,
        scratch_shapes=[
            pltpu.SMEM((steps * count_rows,), jnp.int32),
            pltpu.VMEM((pool_rows, inputs), BF16),
            pltpu.VMEM((inputs, hidden), BF16),
            pltpu.VMEM((pool_rows, outs), BF16),
            pltpu.VMEM((hidden, outs), F32),
            pltpu.VMEM((pool_rows * PITCH, LANES), F32),
            pltpu.VMEM((chunk * PITCH, LANES), F32),
            pltpu.VMEM((chunk * PITCH, LANES), F32),
            pltpu.VMEM((hidden, outs), F32),
            pltpu.VMEM((outs, hidden), F32),
            pltpu.VMEM((outs, hidden), F32),
            pltpu.VMEM((outs, 3 * hidden + outs), BF16),
            pltpu.SemaphoreType.DMA((pool_rows // chunk + 3 + steps,)),
        ],
        compiler_params=pltpu.CompilerParams(vmem_limit_bytes=VMEM_LIMIT),
        name="client",
    )(batch_rows, sample_counts, cluster_ids, features, lower_weight, targets, head_weight)
    arrived = lax.all_to_all(outgoing.reshape(shares * width, 1, LANES), AXES, split_axis=0, concat_axis=0, tiled=True)
    back = pl.pallas_call(
        functools.partial(cluster_kernel, shares=shares),
        out_shape=jax.ShapeDtypeStruct((shares, each, outs), F32),
        in_specs=[vmem],
        out_specs=vmem,
        compiler_params=pltpu.CompilerParams(vmem_limit_bytes=8 << 20),
        name="cluster",
    )(arrived.reshape(shares * width, LANES))
    mine = lax.all_to_all(back, AXES, split_axis=0, concat_axis=0, tiled=True)
    return mine.reshape(head_weight.shape)


def solution(mesh):
    whole = P(AXES, None, None)
    return jax.shard_map(
        on_device,
        mesh=mesh,
        in_specs=(whole, whole, whole, whole, whole, P(AXES), P(AXES)),
        out_specs=whole,
        check_vma=False,
    )
```

```python
import functools

import jax
import jax.numpy as jnp
from jax import lax
from jax.experimental import pallas as pl
from jax.experimental.pallas import tpu as pltpu
from jax.sharding import PartitionSpec as P

LR = 0.5
CLUSTERS = 8
LANES = 128
SUB = 8
PITCH = 9
VMEM_LIMIT = 40 << 20
AXES = ("chip", "board", "cuts")
F32 = jnp.float32
BF16 = jnp.bfloat16


def halves(value):
    high = value.astype(BF16)
    return high, (value - high.astype(F32)).astype(BF16)


def client_kernel(
    rows_hbm, count_ref, cluster_ref, features_ref, lower_ref, targets_ref, head_ref, out_ref,
    rows_ref, places, feat, low, targ, start, pool, picked_a, picked_b,
    first, total, begin, weight, minus, arrived, *, shares, chunk,
):
    pool_rows, hidden = feat.shape[0], low.shape[1]
    steps, count_rows = rows_hbm.shape[1:]
    outs = targ.shape[1]
    blocks, tblocks = hidden // LANES, outs // LANES
    scale = -(LR / count_rows)
    sizes = [chunk] * 2 + [2 * chunk] * ((pool_rows - 2 * chunk) // (2 * chunk))
    sizes += [pool_rows - sum(sizes)] * (sum(sizes) < pool_rows)
    offsets = [sum(sizes[:i]) for i in range(len(sizes))]

    def whole(source, target, i):
        return pltpu.make_async_copy(source, target, arrived.at[i])

    parts = [
        whole(features_ref.at[0, pl.ds(o, n)], feat.at[pl.ds(o, n)], i) for i, (o, n) in enumerate(zip(offsets, sizes))
    ]
    free = len(parts)
    low_copy = whole(lower_ref.at[0], low, free)
    targ_copy = whole(targets_ref.at[0], targ, free + 1)
    head_copy = whole(head_ref.at[0], start, free + 2)
    rows_copy = whole(rows_hbm.at[0], places, free + 3)
    moved = [whole(places.at[s], rows_ref.at[pl.ds(s * count_rows, count_rows)], free + 4 + s) for s in range(steps)]
    low_copy.start()
    for copy in parts[:2]:
        copy.start()
    low_copy.wait()
    parts[2].start()
    rows_copy.start()
    for i, (o, n) in enumerate(zip(offsets, sizes)):
        parts[i].wait()
        if i + 3 < len(parts):
            parts[i + 3].start()
        if i + 4 == len(parts):
            targ_copy.start()
            head_copy.start()
        if i == 2:
            rows_copy.wait()
            places[...] = places[...] * PITCH
        if i == 3:
            for copy in moved:
                copy.start()
        h = jnp.tanh(jnp.dot(feat[o:o + n, :], low[...], preferred_element_type=F32))
        for k in range(blocks):
            pool[pl.ds(o * PITCH + k, n, stride=PITCH), :] = h[:, k * LANES:(k + 1) * LANES]
    targ_copy.wait()
    head_copy.wait()
    for copy in moved:
        copy.wait()
    for k in range(tblocks):
        t = targ[:, k * LANES:(k + 1) * LANES].astype(F32)
        pool[pl.ds(blocks + k, pool_rows, stride=PITCH), :] = t

    per_step = count_rows // chunk

    def pick(i, into):
        for r in range(chunk):
            at = rows_ref[i * chunk + r]
            into[r * PITCH:r * PITCH + SUB, :] = pool[pl.ds(at, SUB), :]

    def picks(source):
        h = jnp.concatenate([source[pl.ds(k, chunk, stride=PITCH), :] for k in range(blocks)], axis=1)
        t = jnp.concatenate([source[pl.ds(blocks + k, chunk, stride=PITCH), :] for k in range(tblocks)], axis=1)
        return (*halves(h), t.astype(BF16))

    def load_weight(value):
        w_high, w_rest = halves(value)
        weight[:outs] = w_high
        weight[outs:] = w_rest

    def errors(h, rest, t):
        dot = functools.partial(lax.dot_general, dimension_numbers=(((1,), (1,)), ((), ())), preferred_element_type=F32)
        both = dot(weight[...], h)
        e = both[:outs] + (both[outs:] + dot(weight[:outs], rest)) + dot(minus[...], t)
        return halves(e)

    start_t = start[...].T
    begin[...] = start_t
    load_weight(start_t)
    row_at = lax.broadcasted_iota(jnp.int32, (outs, outs), 0)
    lane_at = lax.broadcasted_iota(jnp.int32, (outs, outs), 1)
    minus[...] = jnp.where(row_at == lane_at, -1.0, 0.0).astype(BF16)
    pick(0, picked_a)
    pick(1, picked_b)

    for step in range(steps):
        @pl.when(rows_ref[0] >= 0)
        def _():
            for i in range(step * per_step, (step + 1) * per_step, 2):
                h_a, rest_a, t_a = picks(picked_a)
                e_a, d_a = errors(h_a, rest_a, t_a)
                h_b, rest_b, t_b = picks(picked_b)
                e_b, d_b = errors(h_b, rest_b, t_b)
                if i + 2 < steps * per_step:
                    pick(i + 2, picked_a)
                    pick(i + 3, picked_b)
                grad = jnp.dot(
                    jnp.concatenate([e_a, d_a, e_a, e_b, d_b, e_b], axis=1),
                    jnp.concatenate([h_a, h_a, rest_a, h_b, h_b, rest_b], axis=0),
                    preferred_element_type=F32,
                )
                total[...] = grad if i == 0 else total[...] + grad
            if step + 1 < steps:
                load_weight(begin[...] + scale * total[...])

    first[...] = total[...].T

    each = hidden // shares
    width = tblocks * each + 1
    lane = lax.broadcasted_iota(jnp.int32, (1, LANES), 1)
    note = jnp.where(lane < LANES // 2, cluster_ref[0], count_ref[0]).astype(F32)
    for s in range(shares):
        for k in range(tblocks):
            out_ref[s * width + k * each:s * width + (k + 1) * each, :] = (
                first[s * each:(s + 1) * each, k * LANES:(k + 1) * LANES] * scale
            )
        out_ref[(s + 1) * width - 1:(s + 1) * width, :] = note


def cluster_kernel(in_ref, out_ref, *, shares):
    each, outs = out_ref.shape[1], out_ref.shape[2]
    tblocks = outs // LANES
    data = tblocks * each
    width = data + 1
    full = (data, LANES)
    sums = [jnp.zeros(full, F32)] * CLUSTERS
    counts = [jnp.zeros((1, LANES), F32)] * CLUSTERS
    ids = []
    for j in range(shares):
        note = in_ref[(j + 1) * width - 1:(j + 1) * width, :]
        ident = jnp.broadcast_to(note[:, 0:1], (1, LANES))
        count = jnp.broadcast_to(note[:, LANES - 1:LANES], (1, LANES))
        ids.append(ident)
        delta = in_ref[j * width:j * width + data, :]
        for c in range(CLUSTERS):
            weight = jnp.where(ident == c, count, 0.0)
            counts[c] = counts[c] + weight
            sums[c] = sums[c] + weight * delta
    sums = [total / (LR * count) for total, count in zip(sums, counts)]
    for j in range(shares):
        mine = sums[0]
        for c in range(1, CLUSTERS):
            mine = jnp.where(ids[j] == c, sums[c], mine)
        for k in range(tblocks):
            out_ref[j, :, k * LANES:(k + 1) * LANES] = mine[k * each:(k + 1) * each]


def on_device(features, targets, lower_weight, head_weight, batch_rows, sample_counts, cluster_ids):
    shares = lax.axis_size(AXES)
    pool_rows, inputs = features.shape[1:]
    hidden, outs = head_weight.shape[1:]
    chunk = 256
    each = hidden // shares
    tblocks = outs // LANES
    width = tblocks * each + 1
    smem = pl.BlockSpec(memory_space=pltpu.SMEM)
    hbm = pl.BlockSpec(memory_space=pltpu.HBM)
    vmem = pl.BlockSpec(memory_space=pltpu.VMEM)
    steps, count_rows = batch_rows.shape[1:]
    far = functools.partial(pltpu.with_memory_space_constraint, memory_space=pltpu.HBM)
    outgoing = pl.pallas_call(
        functools.partial(client_kernel, shares=shares, chunk=chunk),
        out_shape=jax.ShapeDtypeStruct((shares * width, LANES), F32),
        in_specs=[hbm, smem, smem, hbm, hbm, hbm, hbm],
        out_specs=vmem,
        scratch_shapes=[
            pltpu.SMEM((steps * count_rows,), jnp.int32),
            pltpu.VMEM((steps, count_rows), jnp.int32),
            pltpu.VMEM((pool_rows, inputs), BF16),
            pltpu.VMEM((inputs, hidden), BF16),
            pltpu.VMEM((pool_rows, outs), BF16),
            pltpu.VMEM((hidden, outs), F32),
            pltpu.VMEM((pool_rows * PITCH, LANES), F32),
            pltpu.VMEM((chunk * PITCH, LANES), F32),
            pltpu.VMEM((chunk * PITCH, LANES), F32),
            pltpu.VMEM((hidden, outs), F32),
            pltpu.VMEM((outs, hidden), F32),
            pltpu.VMEM((outs, hidden), F32),
            pltpu.VMEM((2 * outs, hidden), BF16),
            pltpu.VMEM((outs, outs), BF16),
            pltpu.SemaphoreType.DMA((pool_rows // chunk + 4 + steps,)),
        ],
        compiler_params=pltpu.CompilerParams(vmem_limit_bytes=VMEM_LIMIT),
        name="client",
    )(
        far(batch_rows), sample_counts, cluster_ids, far(features), far(lower_weight), far(targets), far(head_weight)
    )
    arrived = lax.all_to_all(outgoing.reshape(shares * width, 1, LANES), AXES, split_axis=0, concat_axis=0, tiled=True)
    back = pl.pallas_call(
        functools.partial(cluster_kernel, shares=shares),
        out_shape=jax.ShapeDtypeStruct((shares, each, outs), F32),
        in_specs=[vmem],
        out_specs=vmem,
        compiler_params=pltpu.CompilerParams(vmem_limit_bytes=8 << 20),
        name="cluster",
    )(arrived.reshape(shares * width, LANES))
    mine = lax.all_to_all(back, AXES, split_axis=0, concat_axis=0, tiled=True)
    return mine.reshape(head_weight.shape)


def solution(mesh):
    whole = P(AXES, None, None)
    return jax.shard_map(
        on_device,
        mesh=mesh,
        in_specs=(whole, whole, whole, whole, whole, P(AXES), P(AXES)),
        out_specs=whole,
        check_vma=False,
    )
```

```python
import functools

import jax
import jax.numpy as jnp
from jax import lax
from jax.experimental import pallas as pl
from jax.experimental.pallas import tpu as pltpu
from jax.sharding import PartitionSpec as P

LR = 0.5
CLUSTERS = 8
LANES = 128
SUB = 8
PITCH = 9
VMEM_LIMIT = 40 << 20
AXES = ("chip", "board", "cuts")
F32 = jnp.float32
BF16 = jnp.bfloat16


def halves(value):
    high = value.astype(BF16)
    return high, (value - high.astype(F32)).astype(BF16)


def client_kernel(
    rows_hbm, count_ref, cluster_ref, features_ref, lower_ref, targets_ref, head_ref, out_ref,
    rows_ref, places, feat, low, targ, start, pool, picked_a, picked_b,
    first, total, begin, weight, arrived, *, shares, chunk,
):
    pool_rows, hidden = feat.shape[0], low.shape[1]
    steps, count_rows = rows_hbm.shape[1:]
    outs = targ.shape[1]
    blocks, tblocks = hidden // LANES, outs // LANES
    scale = -(LR / count_rows)
    sizes = [chunk] * 2 + [2 * chunk] * ((pool_rows - 2 * chunk) // (2 * chunk))
    sizes += [pool_rows - sum(sizes)] * (sum(sizes) < pool_rows)
    offsets = [sum(sizes[:i]) for i in range(len(sizes))]

    def whole(source, target, i):
        return pltpu.make_async_copy(source, target, arrived.at[i])

    parts = [
        whole(features_ref.at[0, pl.ds(o, n)], feat.at[pl.ds(o, n)], i) for i, (o, n) in enumerate(zip(offsets, sizes))
    ]
    free = len(parts)
    low_copy = whole(lower_ref.at[0], low, free)
    targ_copy = whole(targets_ref.at[0], targ, free + 1)
    head_copy = whole(head_ref.at[0], start, free + 2)
    rows_copy = whole(rows_hbm.at[0], places, free + 3)
    moved = [whole(places.at[s], rows_ref.at[pl.ds(s * count_rows, count_rows)], free + 4 + s) for s in range(steps)]
    low_copy.start()
    for copy in parts[:2]:
        copy.start()
    low_copy.wait()
    parts[2].start()
    rows_copy.start()
    for i, (o, n) in enumerate(zip(offsets, sizes)):
        parts[i].wait()
        if i + 3 < len(parts):
            parts[i + 3].start()
        if i + 4 == len(parts):
            targ_copy.start()
            head_copy.start()
        if i == 2:
            rows_copy.wait()
            places[...] = places[...] * PITCH
        if i == 3:
            for copy in moved:
                copy.start()
        h = jnp.tanh(jnp.dot(feat[o:o + n, :], low[...], preferred_element_type=F32))
        for k in range(blocks):
            pool[pl.ds(o * PITCH + k, n, stride=PITCH), :] = h[:, k * LANES:(k + 1) * LANES]
    targ_copy.wait()
    head_copy.wait()
    for copy in moved:
        copy.wait()
    for k in range(tblocks):
        t = targ[:, k * LANES:(k + 1) * LANES].astype(F32)
        pool[pl.ds(blocks + k, pool_rows, stride=PITCH), :] = t

    per_step = count_rows // chunk

    def pick(i, into):
        for r in range(chunk):
            at = rows_ref[i * chunk + r]
            into[r * PITCH:r * PITCH + SUB, :] = pool[pl.ds(at, SUB), :]

    def picks(source):
        h = jnp.concatenate([source[pl.ds(k, chunk, stride=PITCH), :] for k in range(blocks)], axis=1)
        t = jnp.concatenate([source[pl.ds(blocks + k, chunk, stride=PITCH), :] for k in range(tblocks)], axis=1)
        return (*halves(h), t)

    def load_weight(value):
        w_high, w_rest = halves(value)
        weight[:outs] = w_high
        weight[outs:] = w_rest

    def errors(h, rest, t):
        dot = functools.partial(lax.dot_general, dimension_numbers=(((1,), (1,)), ((), ())), preferred_element_type=F32)
        w = weight[...]
        e = dot(jnp.concatenate([w[:outs], w[outs:], w[:outs]], axis=1), jnp.concatenate([h, h, rest], axis=1)) - t.T
        return halves(e)

    start_t = start[...].T
    begin[...] = start_t
    load_weight(start_t)
    pick(0, picked_a)
    pick(1, picked_b)

    for step in range(steps):
        @pl.when(rows_ref[0] >= 0)
        def _():
            for i in range(step * per_step, (step + 1) * per_step, 2):
                h_a, rest_a, t_a = picks(picked_a)
                e_a, d_a = errors(h_a, rest_a, t_a)
                h_b, rest_b, t_b = picks(picked_b)
                e_b, d_b = errors(h_b, rest_b, t_b)
                if i + 2 < steps * per_step:
                    pick(i + 2, picked_a)
                    pick(i + 3, picked_b)
                grad = jnp.dot(
                    jnp.concatenate([e_a, d_a, e_a, e_b, d_b, e_b], axis=1),
                    jnp.concatenate([h_a, h_a, rest_a, h_b, h_b, rest_b], axis=0),
                    preferred_element_type=F32,
                )
                total[...] = grad if i == 0 else total[...] + grad
            if step + 1 < steps:
                load_weight(begin[...] + scale * total[...])

    first[...] = total[...].T

    each = hidden // shares
    width = tblocks * each + 1
    lane = lax.broadcasted_iota(jnp.int32, (1, LANES), 1)
    note = jnp.where(lane < LANES // 2, cluster_ref[0], count_ref[0]).astype(F32)
    for s in range(shares):
        for k in range(tblocks):
            out_ref[s * width + k * each:s * width + (k + 1) * each, :] = (
                first[s * each:(s + 1) * each, k * LANES:(k + 1) * LANES] * scale
            )
        out_ref[(s + 1) * width - 1:(s + 1) * width, :] = note


def cluster_kernel(in_ref, out_ref, *, shares):
    each, outs = out_ref.shape[1], out_ref.shape[2]
    tblocks = outs // LANES
    data = tblocks * each
    width = data + 1
    full = (data, LANES)
    sums = [jnp.zeros(full, F32)] * CLUSTERS
    counts = [jnp.zeros((1, LANES), F32)] * CLUSTERS
    ids = []
    for j in range(shares):
        note = in_ref[(j + 1) * width - 1:(j + 1) * width, :]
        ident = jnp.broadcast_to(note[:, 0:1], (1, LANES))
        count = jnp.broadcast_to(note[:, LANES - 1:LANES], (1, LANES))
        ids.append(ident)
        delta = in_ref[j * width:j * width + data, :]
        for c in range(CLUSTERS):
            weight = jnp.where(ident == c, count, 0.0)
            counts[c] = counts[c] + weight
            sums[c] = sums[c] + weight * delta
    sums = [total / (LR * count) for total, count in zip(sums, counts)]
    for j in range(shares):
        mine = sums[0]
        for c in range(1, CLUSTERS):
            mine = jnp.where(ids[j] == c, sums[c], mine)
        for k in range(tblocks):
            out_ref[j, :, k * LANES:(k + 1) * LANES] = mine[k * each:(k + 1) * each]


def on_device(features, targets, lower_weight, head_weight, batch_rows, sample_counts, cluster_ids):
    shares = lax.axis_size(AXES)
    pool_rows, inputs = features.shape[1:]
    hidden, outs = head_weight.shape[1:]
    chunk = 256
    each = hidden // shares
    tblocks = outs // LANES
    width = tblocks * each + 1
    smem = pl.BlockSpec(memory_space=pltpu.SMEM)
    hbm = pl.BlockSpec(memory_space=pltpu.HBM)
    vmem = pl.BlockSpec(memory_space=pltpu.VMEM)
    steps, count_rows = batch_rows.shape[1:]
    far = functools.partial(pltpu.with_memory_space_constraint, memory_space=pltpu.HBM)
    outgoing = pl.pallas_call(
        functools.partial(client_kernel, shares=shares, chunk=chunk),
        out_shape=jax.ShapeDtypeStruct((shares * width, LANES), F32),
        in_specs=[hbm, smem, smem, hbm, hbm, hbm, hbm],
        out_specs=vmem,
        scratch_shapes=[
            pltpu.SMEM((steps * count_rows,), jnp.int32),
            pltpu.VMEM((steps, count_rows), jnp.int32),
            pltpu.VMEM((pool_rows, inputs), BF16),
            pltpu.VMEM((inputs, hidden), BF16),
            pltpu.VMEM((pool_rows, outs), BF16),
            pltpu.VMEM((hidden, outs), F32),
            pltpu.VMEM((pool_rows * PITCH, LANES), F32),
            pltpu.VMEM((chunk * PITCH, LANES), F32),
            pltpu.VMEM((chunk * PITCH, LANES), F32),
            pltpu.VMEM((hidden, outs), F32),
            pltpu.VMEM((outs, hidden), F32),
            pltpu.VMEM((outs, hidden), F32),
            pltpu.VMEM((2 * outs, hidden), BF16),
            pltpu.SemaphoreType.DMA((pool_rows // chunk + 4 + steps,)),
        ],
        compiler_params=pltpu.CompilerParams(vmem_limit_bytes=VMEM_LIMIT),
        name="client",
    )(
        far(batch_rows), sample_counts, cluster_ids, far(features), far(lower_weight), far(targets), far(head_weight)
    )
    arrived = lax.all_to_all(outgoing.reshape(shares * width, 1, LANES), AXES, split_axis=0, concat_axis=0, tiled=True)
    back = pl.pallas_call(
        functools.partial(cluster_kernel, shares=shares),
        out_shape=jax.ShapeDtypeStruct((shares, each, outs), F32),
        in_specs=[vmem],
        out_specs=vmem,
        compiler_params=pltpu.CompilerParams(vmem_limit_bytes=8 << 20),
        name="cluster",
    )(arrived.reshape(shares * width, LANES))
    mine = lax.all_to_all(back, AXES, split_axis=0, concat_axis=0, tiled=True)
    return mine.reshape(head_weight.shape)


def solution(mesh):
    whole = P(AXES, None, None)
    return jax.shard_map(
        on_device,
        mesh=mesh,
        in_specs=(whole, whole, whole, whole, whole, P(AXES), P(AXES)),
        out_specs=whole,
        check_vma=False,
    )
```

```python
import functools

import jax
import jax.numpy as jnp
from jax import lax
from jax.experimental import pallas as pl
from jax.experimental.pallas import tpu as pltpu
from jax.sharding import PartitionSpec as P

LR = 0.5
CLUSTERS = 8
LANES = 128
SUB = 8
PITCH = 9
VMEM_LIMIT = 40 << 20
AXES = ("chip", "board", "cuts")
F32 = jnp.float32
BF16 = jnp.bfloat16


def halves(value):
    high = value.astype(BF16)
    return high, (value - high.astype(F32)).astype(BF16)


def client_kernel(
    rows_hbm, count_ref, cluster_ref, features_ref, lower_ref, targets_ref, head_ref, out_ref,
    rows_ref, places, feat, low, targ, start, pool, picked_a, picked_b,
    first, total, begin, weight, arrived, *, shares, chunk,
):
    pool_rows, hidden = feat.shape[0], low.shape[1]
    steps, count_rows = rows_hbm.shape[1:]
    outs = targ.shape[1]
    blocks, tblocks = hidden // LANES, outs // LANES
    scale = -(LR / count_rows)
    sizes = [chunk // 2] * 2 + [chunk] * ((pool_rows - chunk) // chunk)
    sizes += [pool_rows - sum(sizes)] * (sum(sizes) < pool_rows)
    offsets = [sum(sizes[:i]) for i in range(len(sizes))]

    def whole(source, target, i):
        return pltpu.make_async_copy(source, target, arrived.at[i])

    parts = [
        whole(features_ref.at[0, pl.ds(o, n)], feat.at[pl.ds(o, n)], i) for i, (o, n) in enumerate(zip(offsets, sizes))
    ]
    free = len(parts)
    low_copy = whole(lower_ref.at[0], low, free)
    targ_copy = whole(targets_ref.at[0], targ, free + 1)
    head_copy = whole(head_ref.at[0], start, free + 2)
    rows_copy = whole(rows_hbm.at[0], places, free + 3)
    moved = [whole(places.at[s], rows_ref.at[pl.ds(s * count_rows, count_rows)], free + 4 + s) for s in range(steps)]
    low_copy.start()
    for copy in parts[:2]:
        copy.start()
    low_copy.wait()
    parts[2].start()
    rows_copy.start()
    for i, (o, n) in enumerate(zip(offsets, sizes)):
        parts[i].wait()
        if i + 3 < len(parts):
            parts[i + 3].start()
        if i + 4 == len(parts):
            targ_copy.start()
            head_copy.start()
        if i == 2:
            rows_copy.wait()
            places[...] = places[...] * PITCH
        if i == 3:
            for copy in moved:
                copy.start()
        h = jnp.tanh(jnp.dot(feat[o:o + n, :], low[...], preferred_element_type=F32))
        for k in range(blocks):
            pool[pl.ds(o * PITCH + k, n, stride=PITCH), :] = h[:, k * LANES:(k + 1) * LANES]
    targ_copy.wait()
    head_copy.wait()
    for copy in moved:
        copy.wait()
    for k in range(tblocks):
        t = targ[:, k * LANES:(k + 1) * LANES].astype(F32)
        pool[pl.ds(blocks + k, pool_rows, stride=PITCH), :] = t

    per_step = count_rows // chunk

    def pick(i, into):
        for r in range(chunk):
            at = rows_ref[i * chunk + r]
            into[r * PITCH:r * PITCH + SUB, :] = pool[pl.ds(at, SUB), :]

    def picks(source):
        h = jnp.concatenate([source[pl.ds(k, chunk, stride=PITCH), :] for k in range(blocks)], axis=1)
        t = jnp.concatenate([source[pl.ds(blocks + k, chunk, stride=PITCH), :] for k in range(tblocks)], axis=1)
        return (*halves(h), t)

    def load_weight(value):
        w_high, w_rest = halves(value)
        weight[:outs] = w_high
        weight[outs:] = w_rest

    def errors(h, rest, t):
        dot = functools.partial(lax.dot_general, dimension_numbers=(((1,), (1,)), ((), ())), preferred_element_type=F32)
        w = weight[...]
        e = dot(jnp.concatenate([w[:outs], w[outs:], w[:outs]], axis=1), jnp.concatenate([h, h, rest], axis=1)) - t.T
        return halves(e)

    start_t = start[...].T
    begin[...] = start_t
    load_weight(start_t)
    pick(0, picked_a)
    pick(1, picked_b)

    for step in range(steps):
        @pl.when(rows_ref[0] >= 0)
        def _():
            for i in range(step * per_step, (step + 1) * per_step, 2):
                h_a, rest_a, t_a = picks(picked_a)
                e_a, d_a = errors(h_a, rest_a, t_a)
                h_b, rest_b, t_b = picks(picked_b)
                e_b, d_b = errors(h_b, rest_b, t_b)
                if i + 2 < steps * per_step:
                    pick(i + 2, picked_a)
                    pick(i + 3, picked_b)
                grad = jnp.dot(
                    jnp.concatenate([e_a, d_a, e_a, e_b, d_b, e_b], axis=1),
                    jnp.concatenate([h_a, h_a, rest_a, h_b, h_b, rest_b], axis=0),
                    preferred_element_type=F32,
                )
                total[...] = grad if i == 0 else total[...] + grad
            if step + 1 < steps:
                load_weight(begin[...] + scale * total[...])

    first[...] = total[...].T

    each = hidden // shares
    width = tblocks * each + 1
    lane = lax.broadcasted_iota(jnp.int32, (1, LANES), 1)
    note = jnp.where(lane < LANES // 2, cluster_ref[0], count_ref[0]).astype(F32)
    for s in range(shares):
        for k in range(tblocks):
            out_ref[s * width + k * each:s * width + (k + 1) * each, :] = (
                first[s * each:(s + 1) * each, k * LANES:(k + 1) * LANES] * scale
            )
        out_ref[(s + 1) * width - 1:(s + 1) * width, :] = note


def cluster_kernel(in_ref, out_ref, *, shares):
    each, outs = out_ref.shape[1], out_ref.shape[2]
    tblocks = outs // LANES
    data = tblocks * each
    width = data + 1
    full = (data, LANES)
    sums = [jnp.zeros(full, F32)] * CLUSTERS
    counts = [jnp.zeros((1, LANES), F32)] * CLUSTERS
    ids = []
    for j in range(shares):
        note = in_ref[(j + 1) * width - 1:(j + 1) * width, :]
        ident = jnp.broadcast_to(note[:, 0:1], (1, LANES))
        count = jnp.broadcast_to(note[:, LANES - 1:LANES], (1, LANES))
        ids.append(ident)
        delta = in_ref[j * width:j * width + data, :]
        for c in range(CLUSTERS):
            weight = jnp.where(ident == c, count, 0.0)
            counts[c] = counts[c] + weight
            sums[c] = sums[c] + weight * delta
    sums = [total / (LR * count) for total, count in zip(sums, counts)]
    for j in range(shares):
        mine = sums[0]
        for c in range(1, CLUSTERS):
            mine = jnp.where(ids[j] == c, sums[c], mine)
        for k in range(tblocks):
            out_ref[j, :, k * LANES:(k + 1) * LANES] = mine[k * each:(k + 1) * each]


def on_device(features, targets, lower_weight, head_weight, batch_rows, sample_counts, cluster_ids):
    shares = lax.axis_size(AXES)
    pool_rows, inputs = features.shape[1:]
    hidden, outs = head_weight.shape[1:]
    chunk = 512
    each = hidden // shares
    tblocks = outs // LANES
    width = tblocks * each + 1
    smem = pl.BlockSpec(memory_space=pltpu.SMEM)
    hbm = pl.BlockSpec(memory_space=pltpu.HBM)
    vmem = pl.BlockSpec(memory_space=pltpu.VMEM)
    steps, count_rows = batch_rows.shape[1:]
    far = functools.partial(pltpu.with_memory_space_constraint, memory_space=pltpu.HBM)
    outgoing = pl.pallas_call(
        functools.partial(client_kernel, shares=shares, chunk=chunk),
        out_shape=jax.ShapeDtypeStruct((shares * width, LANES), F32),
        in_specs=[hbm, smem, smem, hbm, hbm, hbm, hbm],
        out_specs=vmem,
        scratch_shapes=[
            pltpu.SMEM((steps * count_rows,), jnp.int32),
            pltpu.VMEM((steps, count_rows), jnp.int32),
            pltpu.VMEM((pool_rows, inputs), BF16),
            pltpu.VMEM((inputs, hidden), BF16),
            pltpu.VMEM((pool_rows, outs), BF16),
            pltpu.VMEM((hidden, outs), F32),
            pltpu.VMEM((pool_rows * PITCH, LANES), F32),
            pltpu.VMEM((chunk * PITCH, LANES), F32),
            pltpu.VMEM((chunk * PITCH, LANES), F32),
            pltpu.VMEM((hidden, outs), F32),
            pltpu.VMEM((outs, hidden), F32),
            pltpu.VMEM((outs, hidden), F32),
            pltpu.VMEM((2 * outs, hidden), BF16),
            pltpu.SemaphoreType.DMA((pool_rows // chunk + 8 + steps,)),
        ],
        compiler_params=pltpu.CompilerParams(vmem_limit_bytes=VMEM_LIMIT),
        name="client",
    )(
        far(batch_rows), sample_counts, cluster_ids, far(features), far(lower_weight), far(targets), far(head_weight)
    )
    arrived = lax.all_to_all(outgoing.reshape(shares * width, 1, LANES), AXES, split_axis=0, concat_axis=0, tiled=True)
    back = pl.pallas_call(
        functools.partial(cluster_kernel, shares=shares),
        out_shape=jax.ShapeDtypeStruct((shares, each, outs), F32),
        in_specs=[vmem],
        out_specs=vmem,
        compiler_params=pltpu.CompilerParams(vmem_limit_bytes=8 << 20),
        name="cluster",
    )(arrived.reshape(shares * width, LANES))
    mine = lax.all_to_all(back, AXES, split_axis=0, concat_axis=0, tiled=True)
    return mine.reshape(head_weight.shape)


def solution(mesh):
    whole = P(AXES, None, None)
    return jax.shard_map(
        on_device,
        mesh=mesh,
        in_specs=(whole, whole, whole, whole, whole, P(AXES), P(AXES)),
        out_specs=whole,
        check_vma=False,
    )
```

```python
import functools

import jax
import jax.numpy as jnp
from jax import lax
from jax.experimental import pallas as pl
from jax.experimental.pallas import tpu as pltpu
from jax.sharding import PartitionSpec as P

LR = 0.5
CLUSTERS = 8
LANES = 128
SUB = 8
PITCH = 9
VMEM_LIMIT = 40 << 20
AXES = ("chip", "board", "cuts")
F32 = jnp.float32
BF16 = jnp.bfloat16


def halves(value):
    high = value.astype(BF16)
    return high, (value - high.astype(F32)).astype(BF16)


def client_kernel(
    rows_hbm, count_ref, cluster_ref, features_ref, lower_ref, targets_ref, head_ref, out_ref,
    rows_ref, places, feat, low, targ, start, pool, picked_a, picked_b,
    first, total, begin, weight, arrived, *, shares, chunk,
):
    pool_rows, hidden = feat.shape[0], low.shape[1]
    steps, count_rows = rows_hbm.shape[1:]
    outs = targ.shape[1]
    blocks, tblocks = hidden // LANES, outs // LANES
    scale = -(LR / count_rows)
    sizes = [chunk // 2] * 2 + [chunk] * ((pool_rows - chunk) // chunk)
    sizes += [pool_rows - sum(sizes)] * (sum(sizes) < pool_rows)
    offsets = [sum(sizes[:i]) for i in range(len(sizes))]

    def whole(source, target, i):
        return pltpu.make_async_copy(source, target, arrived.at[i])

    parts = [
        whole(features_ref.at[0, pl.ds(o, n)], feat.at[pl.ds(o, n)], i) for i, (o, n) in enumerate(zip(offsets, sizes))
    ]
    free = len(parts)
    low_copy = whole(lower_ref.at[0], low, free)
    targ_copy = whole(targets_ref.at[0], targ, free + 1)
    head_copy = whole(head_ref.at[0], start, free + 2)
    rows_copy = whole(rows_hbm.at[0], places, free + 3)
    moved = [whole(places.at[s], rows_ref.at[pl.ds(s * count_rows, count_rows)], free + 4 + s) for s in range(steps)]
    low_copy.start()
    for copy in parts[:2]:
        copy.start()
    low_copy.wait()
    parts[2].start()
    rows_copy.start()
    for i, (o, n) in enumerate(zip(offsets, sizes)):
        parts[i].wait()
        if i + 3 < len(parts):
            parts[i + 3].start()
        if i + 4 == len(parts):
            targ_copy.start()
            head_copy.start()
        if i == 2:
            rows_copy.wait()
            places[...] = places[...] * PITCH
        if i == 3:
            for copy in moved:
                copy.start()
        h = jnp.tanh(jnp.dot(feat[o:o + n, :], low[...], preferred_element_type=F32))
        for k in range(blocks):
            pool[pl.ds(o * PITCH + k, n, stride=PITCH), :] = h[:, k * LANES:(k + 1) * LANES]
    targ_copy.wait()
    head_copy.wait()
    for copy in moved:
        copy.wait()
    for k in range(tblocks):
        t = targ[:, k * LANES:(k + 1) * LANES].astype(F32)
        pool[pl.ds(blocks + k, pool_rows, stride=PITCH), :] = t

    per_step = count_rows // chunk

    def pick(i, into):
        for r in range(chunk):
            at = rows_ref[i * chunk + r]
            into[r * PITCH:r * PITCH + SUB, :] = pool[pl.ds(at, SUB), :]

    def picks(source):
        h = jnp.concatenate([source[pl.ds(k, chunk, stride=PITCH), :] for k in range(blocks)], axis=1)
        t = jnp.concatenate([source[pl.ds(blocks + k, chunk, stride=PITCH), :] for k in range(tblocks)], axis=1)
        return (*halves(h), t)

    def load_weight(value):
        w_high, w_rest = halves(value)
        weight[:outs] = w_high
        weight[outs:] = w_rest

    def errors(h, rest, t):
        dot = functools.partial(lax.dot_general, dimension_numbers=(((1,), (1,)), ((), ())), preferred_element_type=F32)
        w = weight[...]
        e = dot(jnp.concatenate([w[:outs], w[outs:], w[:outs]], axis=1), jnp.concatenate([h, h, rest], axis=1)) - t.T
        return halves(e)

    start_t = start[...].T
    begin[...] = start_t
    load_weight(start_t)
    pick(0, picked_a)
    pick(1, picked_b)

    for step in range(steps):
        @pl.when(rows_ref[0] >= 0)
        def _():
            for i in range(step * per_step, (step + 1) * per_step, 2):
                h_a, rest_a, t_a = picks(picked_a)
                e_a, d_a = errors(h_a, rest_a, t_a)
                h_b, rest_b, t_b = picks(picked_b)
                e_b, d_b = errors(h_b, rest_b, t_b)
                if i + 2 < steps * per_step:
                    pick(i + 2, picked_a)
                    pick(i + 3, picked_b)
                grad = jnp.dot(
                    jnp.concatenate([e_a, d_a, e_a, e_b, d_b, e_b], axis=1),
                    jnp.concatenate([h_a, h_a, rest_a, h_b, h_b, rest_b], axis=0),
                    preferred_element_type=F32,
                )
                total[...] = grad if i == 0 else total[...] + grad
            if step + 1 < steps:
                load_weight(begin[...] + scale * total[...])

    delta = (total[...] * scale).T

    each = hidden // shares
    width = tblocks * each + 1
    lane = lax.broadcasted_iota(jnp.int32, (1, LANES), 1)
    note = jnp.where(lane < LANES // 2, cluster_ref[0], count_ref[0]).astype(F32)
    for s in range(shares):
        for k in range(tblocks):
            out_ref[s * width + k * each:s * width + (k + 1) * each, :] = (
                delta[s * each:(s + 1) * each, k * LANES:(k + 1) * LANES]
            )
        out_ref[(s + 1) * width - 1:(s + 1) * width, :] = note


def cluster_kernel(in_ref, out_ref, *, shares):
    each, outs = out_ref.shape[1], out_ref.shape[2]
    tblocks = outs // LANES
    data = tblocks * each
    width = data + 1
    full = (data, LANES)
    sums = [jnp.zeros(full, F32)] * CLUSTERS
    counts = [jnp.zeros((1, LANES), F32)] * CLUSTERS
    ids = []
    for j in range(shares):
        note = in_ref[(j + 1) * width - 1:(j + 1) * width, :]
        ident = jnp.broadcast_to(note[:, 0:1], (1, LANES))
        count = jnp.broadcast_to(note[:, LANES - 1:LANES], (1, LANES))
        ids.append(ident)
        delta = in_ref[j * width:j * width + data, :]
        for c in range(CLUSTERS):
            weight = jnp.where(ident == c, count, 0.0)
            counts[c] = counts[c] + weight
            sums[c] = sums[c] + weight * delta
    sums = [total * (1.0 / (LR * count)) for total, count in zip(sums, counts)]
    for j in range(shares):
        mine = sums[0]
        for c in range(1, CLUSTERS):
            mine = jnp.where(ids[j] == c, sums[c], mine)
        for k in range(tblocks):
            out_ref[j, :, k * LANES:(k + 1) * LANES] = mine[k * each:(k + 1) * each]


def on_device(features, targets, lower_weight, head_weight, batch_rows, sample_counts, cluster_ids):
    shares = lax.axis_size(AXES)
    pool_rows, inputs = features.shape[1:]
    hidden, outs = head_weight.shape[1:]
    chunk = 512
    each = hidden // shares
    tblocks = outs // LANES
    width = tblocks * each + 1
    smem = pl.BlockSpec(memory_space=pltpu.SMEM)
    hbm = pl.BlockSpec(memory_space=pltpu.HBM)
    vmem = pl.BlockSpec(memory_space=pltpu.VMEM)
    steps, count_rows = batch_rows.shape[1:]
    far = functools.partial(pltpu.with_memory_space_constraint, memory_space=pltpu.HBM)
    outgoing = pl.pallas_call(
        functools.partial(client_kernel, shares=shares, chunk=chunk),
        out_shape=jax.ShapeDtypeStruct((shares * width, LANES), F32),
        in_specs=[hbm, smem, smem, hbm, hbm, hbm, hbm],
        out_specs=vmem,
        scratch_shapes=[
            pltpu.SMEM((steps * count_rows,), jnp.int32),
            pltpu.VMEM((steps, count_rows), jnp.int32),
            pltpu.VMEM((pool_rows, inputs), BF16),
            pltpu.VMEM((inputs, hidden), BF16),
            pltpu.VMEM((pool_rows, outs), BF16),
            pltpu.VMEM((hidden, outs), F32),
            pltpu.VMEM((pool_rows * PITCH, LANES), F32),
            pltpu.VMEM((chunk * PITCH, LANES), F32),
            pltpu.VMEM((chunk * PITCH, LANES), F32),
            pltpu.VMEM((hidden, outs), F32),
            pltpu.VMEM((outs, hidden), F32),
            pltpu.VMEM((outs, hidden), F32),
            pltpu.VMEM((2 * outs, hidden), BF16),
            pltpu.SemaphoreType.DMA((pool_rows // chunk + 8 + steps,)),
        ],
        compiler_params=pltpu.CompilerParams(vmem_limit_bytes=VMEM_LIMIT),
        name="client",
    )(
        far(batch_rows), sample_counts, cluster_ids, far(features), far(lower_weight), far(targets), far(head_weight)
    )
    arrived = lax.all_to_all(outgoing.reshape(shares * width, 1, LANES), AXES, split_axis=0, concat_axis=0, tiled=True)
    back = pl.pallas_call(
        functools.partial(cluster_kernel, shares=shares),
        out_shape=jax.ShapeDtypeStruct((shares, each, outs), F32),
        in_specs=[vmem],
        out_specs=vmem,
        compiler_params=pltpu.CompilerParams(vmem_limit_bytes=8 << 20),
        name="cluster",
    )(arrived.reshape(shares * width, LANES))
    mine = lax.all_to_all(back, AXES, split_axis=0, concat_axis=0, tiled=True)
    return mine.reshape(head_weight.shape)


def solution(mesh):
    whole = P(AXES, None, None)
    return jax.shard_map(
        on_device,
        mesh=mesh,
        in_specs=(whole, whole, whole, whole, whole, P(AXES), P(AXES)),
        out_specs=whole,
        check_vma=False,
    )
```
